16 devices in a mesh: dp: 1, tp: 16 (over x, y, z, core).
Axes of the slice: x: 2, y: 2, z: 2, core: 2. Of those that a mesh axis runs over, the one named last changes fastest.
Arguments:
- x: bfloat16 [5632, 3072], P(('dp', 'tp'))
- w: bfloat16 [3072, 32768], P(None, 'tp')
- label: int32 [5632], P(('dp', 'tp'))
Outputs:
- output 1: float32 [5632], P(('dp', 'tp'))
- output 2: bfloat16 [5632, 3072], P(('dp', 'tp'))
- output 3: bfloat16 [3072, 32768], P('dp', 'tp')
All inputs are finite; a program needn't handle non-finite values.
Results may differ from the reference program's by a relative error of at most 0.012.
Values are sent between devices in bfloat16 or wider.
A program may use at most 2 GiB of HBM per device.

```python
import jax
import jax.numpy as jnp

ROWS = 5632
D = 3072
VOCAB = 32768


def setup_inputs(seed: int = 0, part: int = 0) -> dict:
    kx, kw, kl = jax.random.split(jax.random.key(seed), 3)
    kx, kl = (jax.random.fold_in(k, part) for k in (kx, kl))
    return {
        "x": jax.random.normal(kx, (ROWS, D), jnp.float32).astype(jnp.bfloat16),
        "w": (jax.random.normal(kw, (D, VOCAB), jnp.float32) * (4.0 / D) ** 0.5).astype(jnp.bfloat16),
        "label": jax.random.randint(kl, (ROWS,), 0, VOCAB, jnp.int32),
    }


def reference(x, w, label):
    logits = jnp.dot(x, w, preferred_element_type=jnp.float32)
    top = jnp.max(logits, -1, keepdims=True)
    e = jnp.exp(logits - top)
    total = jnp.sum(e, -1, keepdims=True)
    hit = label[:, None] == jnp.arange(VOCAB, dtype=jnp.int32)[None, :]
    loss = jnp.log(total[:, 0]) + top[:, 0] - jnp.sum(jnp.where(hit, logits, 0.0), -1)
    by_logits = (e / total - hit.astype(jnp.float32)).astype(jnp.bfloat16)
    by_x = jnp.dot(by_logits, w.T, preferred_element_type=jnp.float32).astype(jnp.bfloat16)
    by_w = jnp.dot(x.T, by_logits, preferred_element_type=jnp.float32).astype(jnp.bfloat16)
    return loss, by_x, by_w
```

```python
import jax
import jax.numpy as jnp
from jax import lax
from jax.experimental import pallas as pl
from jax.experimental.pallas import tpu as pltpu
from jax.sharding import PartitionSpec as P

F32, BF16, I32 = jnp.float32, jnp.bfloat16, jnp.int32
R, D, C = 352, 3072, 2048
PO, PS = (0, 128, 240), (128, 112, 112)
AXES = (8, 4, 2)
NB = 16
MB = 256
DONE = 6
VMEM_LIMIT = 67_000_000


def flip(me, v):
    return v * (1 - 2 * ((me // v) % 2))


def place():
    me = lax.axis_index("tp")
    return me, me + flip(me, 1), [me + flip(me, v) for v in AXES]


def origin(me, s, k, j):
    q = me + k * flip(me, 1)
    for b in range(3):
        q = q + ((s // (1 << b)) % 2) * flip(me, AXES[(j + b) % 3])
    return q


def order(i):
    return jnp.where(i == 3, 4, jnp.where(i == 4, 3, i))


def rc(src, dst, ss, rs, dev):
    return pltpu.make_async_remote_copy(
        src_ref=src, dst_ref=dst, send_sem=ss, recv_sem=rs, device_id={"tp": dev}, device_id_type=pl.DeviceIdType.MESH
    )


def rows(j):
    return pl.ds(PO[j], PS[j])


def eye():
    return lax.broadcasted_iota(I32, (128, 128), 0) == lax.broadcasted_iota(I32, (128, 128), 1)


def to_column(row):
    return jnp.sum(jnp.where(eye(), row, 0.0), 1, keepdims=True)


def to_row(column, n):
    return jnp.sum(jnp.where(eye()[:n], column, 0.0), 0, keepdims=True)


def fill_columns(dst, tile, j, row, shift=0.0):
    col = to_column(tile[row : row + 1, :].astype(F32) - shift)
    dst[rows(j), :] = jnp.broadcast_to(col, (128, 128))[: PS[j]]


def first_kernel(
    x_hbm, w_hbm, lab_ref,
    z_hbm, xr_hbm, loss_ref, st_out, lab_out,
    xv, w, zb, labc, mc, sc, rcol, stile, strecv, st_all, lab_all,
    isend, irecv, dsend, drecv, zsem, xsem, lsend, lrecv, ssend, srecv, tsend, trecv, insem,
):
    me, partner, nbr = place()
    base = me * C
    load_x = pltpu.make_async_copy(x_hbm, xv.at[0, 0], insem.at[0])
    load_w = pltpu.make_async_copy(w_hbm, w, insem.at[1])
    load_x.start()
    load_w.start()

    barrier = pltpu.get_barrier_semaphore()

    @pl.loop(1, NB)
    def _(t):
        pl.semaphore_signal(barrier, inc=1, device_id={"tp": (me + t) % NB}, device_id_type=pl.DeviceIdType.MESH)

    pl.semaphore_wait(barrier, NB - 1)

    def label_copy(t):
        return rc(lab_ref, lab_all.at[me], lsend.at[t], lrecv.at[me], (me + t) % NB)

    def label_from(t):
        q = (me + t) % NB
        return rc(lab_ref, lab_all.at[q], lsend.at[t], lrecv.at[q], q)

    def ici(s, b, j):
        t = s + (1 << b)
        return rc(xv.at[s, 0, rows(j)], xv.at[t, 0, rows(j)], isend.at[t, j], irecv.at[t, j], nbr[(j + b) % 3])

    def d2d(s):
        return rc(xv.at[s, 0], xv.at[s, 1], dsend.at[s], drecv.at[s], partner)

    def z_out(s, k, par):
        return pltpu.make_async_copy(zb.at[par], z_hbm.at[pl.ds((2 * s + k) * R, R)], zsem.at[par])

    def x_out(s, k):
        return pltpu.make_async_copy(xv.at[s, k], xr_hbm.at[pl.ds((2 * s + k) * R, R)], xsem.at[s, k])

    def stat_copy(s, k, j):
        n = 2 * s + k
        q = origin(me, s, k, j)
        return rc(stile.at[n, j], strecv.at[me, j], ssend.at[n, j], srecv.at[me, j], q)

    @pl.loop(1, NB)
    def _(t):
        label_copy(t).start()

    lab_all[me] = lab_ref[...]
    load_x.wait()

    @pl.loop(0, 8)
    def _(i):
        s = order(i)
        for k in range(2):
            if k == 0:

                @pl.when(i > 0)
                def _():
                    for j in range(3):
                        rc(xv.at[s, 0, rows(j)], xv.at[s, 0, rows(j)], isend.at[s, j], irecv.at[s, j], nbr[j]).wait_recv()

                for b in range(3):

                    @pl.when(s < (1 << b))
                    def _():
                        for j in range(3):
                            ici(s, b, j).start()

                d2d(s).start()

                @pl.when(i == 0)
                def _():
                    load_w.wait()

                    @pl.loop(1, NB)
                    def _(t):
                        label_from(t).wait_recv()
            else:
                d2d(s).wait_recv()
            x_out(s, k).start()

            @pl.when(i > 0)
            def _():
                z_out(0, k, k).wait()

            zb[k] = jnp.dot(xv[s, k], w[...], preferred_element_type=F32)
            for j in range(3):
                fill_columns(labc, lab_all[origin(me, s, k, j)], j, j, base.astype(F32))

            @pl.loop(0, 4)
            def _(n):
                r = pl.ds(pl.multiple_of(n * 88, 8), 88)
                high = zb[k, r, 0:128]
                for c in range(1, C // 128):
                    high = jnp.maximum(high, zb[k, r, c * 128 : (c + 1) * 128])
                high = jnp.max(high, 1, keepdims=True)
                lab = labc[r, :]
                lane = lax.broadcasted_iota(I32, (88, 128), 1).astype(F32)
                sums = jnp.zeros((88, 128), F32)
                right = jnp.zeros((88, 128), F32)
                for c in range(C // 128):
                    z = zb[k, r, c * 128 : (c + 1) * 128]
                    sums = sums + jnp.exp(z - high)
                    right = right + jnp.where(lane == lab - c * 128.0, z, 0.0)
                mc[r, :] = jnp.broadcast_to(high, (88, 128))
                sc[r, :] = jnp.broadcast_to(jnp.sum(sums, 1, keepdims=True), (88, 128))
                rcol[r, :] = jnp.broadcast_to(jnp.sum(right, 1, keepdims=True), (88, 128))

            z_out(s, k, k).start()
            for j in range(3):
                for n, ref in enumerate((mc, sc, rcol)):
                    stile[2 * s + k, j, n : n + 1, :] = to_row(ref[rows(j), :], PS[j])
            if k == 0:

                @pl.when(i == 0)
                def _():
                    for j in range(3):
                        strecv[me, j] = stile[0, j]

                @pl.when(i > 0)
                def _():
                    for j in range(3):
                        stat_copy(s, k, j).start()
            else:
                for j in range(3):
                    stat_copy(s, k, j).start()

    @pl.loop(1, NB)
    def _(t):
        q = (me + t) % NB
        for j in range(3):
            rc(strecv.at[q, j], strecv.at[q, j], ssend.at[0, j], srecv.at[q, j], q).wait_recv()

    for j in range(3):
        tiles = [strecv[q, j] for q in range(NB)]
        top = tiles[0][0:1]
        for t in tiles[1:]:
            top = jnp.maximum(top, t[0:1])
        total = jnp.zeros((1, 128), F32)
        right = jnp.zeros((1, 128), F32)
        for t in tiles:
            total = total + t[1:2] * jnp.exp(t[0:1] - top)
            right = right + t[2:3]
        loss_ref[j : j + 1, :] = jnp.log(total) + top - right
        st_all[me, j : j + 1, :] = top
        st_all[me, j + 3 : j + 4, :] = 1.0 / total

    def top_copy(t):
        return rc(st_all.at[me], st_all.at[me], tsend.at[t], trecv.at[me], (me + t) % NB)

    def top_from(t):
        q = (me + t) % NB
        return rc(st_all.at[q], st_all.at[q], tsend.at[t], trecv.at[q], q)

    @pl.loop(1, NB)
    def _(t):
        top_copy(t).start()

    lab_out[...] = lab_all[...]
    for s in range(8):
        for k in range(2):
            x_out(s, k).wait()
    for k in range(2):
        z_out(0, k, k).wait()
    for b in range(3):
        for s in range(1 << b):
            for j in range(3):
                ici(s, b, j).wait_send()

    @pl.loop(0, 8)
    def _(s):
        d2d(s).wait_send()

    @pl.loop(1, NB)
    def _(n):
        for j in range(3):
            stat_copy(n // 2, n % 2, j).wait_send()

    @pl.loop(1, NB)
    def _(t):
        label_copy(t).wait_send()
        top_copy(t).wait_send()
        top_from(t).wait_recv()

    st_out[...] = st_all[...]


def by_w_block(xb, g, ob):
    for c in range(4):
        ob[:, c * 512 : (c + 1) * 512] = lax.dot_general(
            xb[...], g[:, c * 512 : (c + 1) * 512], (((0,), (0,)), ((), ())), preferred_element_type=F32
        ).astype(BF16)


def second_kernel(
    z_hbm, xr_hbm, w_hbm, st_ref, lab_ref,
    byx, g_hbm, bw, dbuf, ibuf,
    w, g, zin, pool, acc, xb, ob, topc, invc, labc,
    insem, zsem, dsend, drecv, isend, irecv, gsem, lsem, xsem, osem,
):
    me, partner, nbr = place()
    base = me * C
    load_w = pltpu.make_async_copy(w_hbm, w, insem.at[0])

    def z_in(s, k, h):
        return pltpu.make_async_copy(z_hbm.at[pl.ds((2 * s + k) * R + h * 88, 88)], zin.at[h % 2], zsem.at[h % 2])

    z_in(7, 1, 0).start()
    z_in(7, 1, 1).start()
    load_w.start()
    barrier = pltpu.get_barrier_semaphore()
    for q in (partner, *nbr):
        pl.semaphore_signal(barrier, inc=1, device_id={"tp": q}, device_id_type=pl.DeviceIdType.MESH)
    pl.semaphore_wait(barrier, 4)

    def d2d(s, p):
        return rc(pool.at[p], dbuf.at[s], dsend.at[p], drecv.at[s], partner)

    def ici(s, b, p, j):
        return rc(pool.at[p, rows(j)], ibuf.at[s, rows(j)], isend.at[p, j], irecv.at[s, j], nbr[(j + b) % 3])

    def fetch(src, p):
        return pltpu.make_async_copy(src, pool.at[p], lsem.at[p])

    def g_out(s, k):
        n = pl.ds((2 * s + k) * R, R)
        return pltpu.make_async_copy(g.at[n], g_hbm.at[n], gsem.at[s, k])

    def x_in(m):
        return pltpu.make_async_copy(xr_hbm.at[:, pl.ds(m * MB, MB)], xb.at[m % 2], xsem.at[m % 2])

    def bw_out(m):
        return pltpu.make_async_copy(ob.at[m % 2], bw.at[pl.ds(m * MB, MB)], osem.at[m % 2])

    def gradient(s, k, nxt):
        for j in range(3):
            q = origin(me, s, k, j)
            fill_columns(topc, st_ref[q], j, j)
            fill_columns(invc, st_ref[q], j, j + 3)
            fill_columns(labc, lab_ref[q], j, j, base.astype(F32))

        @pl.loop(0, 4)
        def _(h):
            z_in(s, k, h).wait()
            r = pl.ds(pl.multiple_of(h * 88, 8), 88)
            to = pl.ds(pl.multiple_of((2 * s + k) * R + h * 88, 8), 88)
            top, inv, lab = topc[r, :], invc[r, :], labc[r, :]
            lane = lax.broadcasted_iota(I32, (88, 128), 1).astype(F32)
            for c in range(C // 128):
                e = jnp.exp(zin[h % 2, :, c * 128 : (c + 1) * 128] - top) * inv
                hit = jnp.where(lane == lab - c * 128.0, 1.0, 0.0)
                g[to, c * 128 : (c + 1) * 128] = (e - hit).astype(BF16)

            @pl.when(h < 2)
            def _():
                z_in(s, k, h + 2).start()

            @pl.when(h >= 2)
            def _():
                nxt(h - 2)

        g_out(s, k).start()

    def term(s, k, n):
        return lax.dot_general(
            g[pl.ds(pl.multiple_of((2 * s + k) * R, R), R), :],
            w[pl.ds(pl.multiple_of(n * 1536, 1536), 1536), :],
            (((1,), (1,)), ((), ())),
            preferred_element_type=F32,
        )

    def wait_slot(s):
        for j in range(3):
            rc(ibuf.at[s, rows(j)], ibuf.at[s, rows(j)], isend.at[2, j], irecv.at[s, j], nbr[j]).wait_recv()

    @pl.loop(0, 8)
    def _(i):
        s = 7 - order(i)
        prev = 7 - order(jnp.maximum(i - 1, 0))
        after = 7 - order(jnp.minimum(i + 1, 7))
        a = i % 2
        p = 2 + (i + 2) % 3

        def next_half(h):
            z_in(s, 0, h).start()

        def next_slot(h):
            @pl.when(i < 7)
            def _():
                z_in(after, 1, h).start()

        gradient(s, 1, next_half)

        @pl.when(i == 0)
        def _():
            load_w.wait()

        @pl.when(i > 1)
        def _():
            d2d(0, a).wait_send()

        @pl.when(i > 3)
        def _():
            for j in range(3):
                ici(0, 0, p, j).wait_send()

        @pl.when(i > 0)
        def _():
            d2d(prev, 0).wait_recv()
            fetch(dbuf.at[prev], 5).start()

            @pl.when(prev < 4)
            def _():
                wait_slot(prev + 4)
                fetch(ibuf.at[prev + 4], 6).start()

            @pl.when(prev < 2)
            def _():
                wait_slot(prev + 2)
                fetch(ibuf.at[prev + 2], p).start()

        @pl.loop(0, 2)
        def _(n):
            c = pl.ds(pl.multiple_of(n * 1536, 1536), 1536)
            pool[a, :, c] = term(s, 1, n).astype(BF16)

        d2d(s, a).start()
        gradient(s, 0, next_slot)

        @pl.when(i > 0)
        def _():
            fetch(dbuf.at[prev], 5).wait()

            @pl.when(prev < 4)
            def _():
                fetch(ibuf.at[prev + 4], 6).wait()

            @pl.when(prev < 2)
            def _():
                fetch(ibuf.at[prev + 2], p).wait()

            @pl.loop(0, 2)
            def _(n):
                c = pl.ds(pl.multiple_of(n * 1536, 1536), 1536)
                acc[...] = term(prev, 0, n) + pool[5, :, c].astype(F32)

                @pl.when(prev < 4)
                def _():
                    acc[...] += pool[6, :, c].astype(F32)

                @pl.when(prev < 2)
                def _():
                    acc[...] += pool[p, :, c].astype(F32)

                pool[p, :, c] = acc[...].astype(BF16)

            @pl.when(prev >= 4)
            def _():
                for j in range(3):
                    ici(prev, 2, p, j).start()

            @pl.when((prev >= 2) & (prev < 4))
            def _():
                for j in range(3):
                    ici(prev, 1, p, j).start()

            @pl.when(prev == 1)
            def _():
                for j in range(3):
                    ici(prev, 0, p, j).start()

    x_in(0).start()
    x_in(1).start()

    @pl.loop(0, DONE)
    def _(m):
        x_in(m).wait()

        @pl.when(m > 1)
        def _():
            bw_out(m - 2).wait()

        by_w_block(xb.at[m % 2], g, ob.at[m % 2])
        bw_out(m).start()

        @pl.when(m + 2 < DONE)
        def _():
            x_in(m + 2).start()

    for a in range(2):
        d2d(0, a).wait_send()
    d2d(0, 0).wait_recv()
    fetch(dbuf.at[0], 5).start()
    for s, p in ((4, 6), (2, 0), (1, 1)):
        wait_slot(s)
        fetch(ibuf.at[s], p).start()
    for p in (5, 6, 0, 1):
        fetch(dbuf.at[0], p).wait()

    @pl.loop(0, 2)
    def _(n):
        c = pl.ds(pl.multiple_of(n * 1536, 1536), 1536)
        acc[...] = term(0, 0, n)
        for p in (5, 6, 0, 1):
            acc[...] += pool[p, :, c].astype(F32)
        pool[5, :, c] = acc[...].astype(BF16)

    out = pltpu.make_async_copy(pool.at[5], byx, lsem.at[5])
    out.start()
    out.wait()

    for p in (2, 3, 4):
        for j in range(3):
            ici(0, 0, p, j).wait_send()
    for s in range(8):
        for k in range(2):
            g_out(s, k).wait()
    for m in (DONE - 2, DONE - 1):
        bw_out(m).wait()


def third_kernel(g_hbm, xr_hbm, part_hbm, bw, g, xb, ob, part, acc, gsem, xsem, osem, psem):
    blocks = D // MB

    def g_in(n):
        r = pl.ds(n * 1408, 1408)
        return pltpu.make_async_copy(g_hbm.at[r], g.at[r], gsem.at[n])

    def x_in(m):
        return pltpu.make_async_copy(xr_hbm.at[:, pl.ds(m * MB, MB)], xb.at[m % 2], xsem.at[m % 2])

    def bw_out(m):
        return pltpu.make_async_copy(ob.at[m % 2], bw.at[pl.ds(m * MB, MB)], osem.at[m % 2])

    p_in = pltpu.make_async_copy(part_hbm, part, psem.at[0])
    p_out = pltpu.make_async_copy(part, bw.at[pl.ds(0, DONE * MB)], psem.at[1])
    x_in(DONE).start()
    for n in range(4):
        g_in(n).start()
    x_in(DONE + 1).start()
    p_in.start()

    x_in(DONE).wait()
    for n in range(4):
        g_in(n).wait()
        r = pl.ds(n * 1408, 1408)
        for c in range(4):
            cols = pl.ds(c * 512, 512)
            t = lax.dot_general(
                xb[DONE % 2, r, :], g[r, cols], (((0,), (0,)), ((), ())), preferred_element_type=F32
            )
            if n == 0:
                acc[:, cols] = t
            else:
                acc[:, cols] += t
    ob[DONE % 2] = acc[...].astype(BF16)
    bw_out(DONE).start()
    x_in(DONE + 2).start()
    p_in.wait()
    p_out.start()

    @pl.loop(DONE + 1, blocks)
    def _(m):
        x_in(m).wait()

        @pl.when(m > DONE + 1)
        def _():
            bw_out(m - 2).wait()

        by_w_block(xb.at[m % 2], g, ob.at[m % 2])
        bw_out(m).start()

        @pl.when(m + 2 < blocks)
        def _():
            x_in(m + 2).start()

    for m in (blocks - 2, blocks - 1):
        bw_out(m).wait()
    p_out.wait()


ANY = pl.BlockSpec(memory_space=pl.ANY)
VM = pl.BlockSpec(memory_space=pltpu.VMEM)


def params(n=None):
    if n is None:
        return pltpu.CompilerParams(vmem_limit_bytes=VMEM_LIMIT)
    return pltpu.CompilerParams(vmem_limit_bytes=VMEM_LIMIT, collective_id=n, has_side_effects=True)


def S(shape, dtype):
    return jax.ShapeDtypeStruct(shape, dtype)


def pieces(v):
    out = [jnp.pad(v[o : o + n], (0, 128 - n)) for o, n in zip(PO, PS)]
    return jnp.pad(jnp.stack(out), ((0, 5), (0, 0)))


def solution(mesh):
    DMA = pltpu.SemaphoreType.DMA
    rows_all = NB * R

    def step(x, w, label):
        z, xr, loss, st, lab = pl.pallas_call(
            first_kernel,
            out_shape=(
                S((rows_all, C), F32),
                S((rows_all, D), BF16),
                S((8, 128), F32),
                S((NB, 8, 128), F32),
                S((NB, 8, 128), I32),
            ),
            in_specs=[ANY, ANY, VM],
            out_specs=(ANY, ANY, VM, VM, VM),
            scratch_shapes=[
                pltpu.VMEM((8, 2, R, D), BF16),
                pltpu.VMEM((D, C), BF16),
                pltpu.VMEM((2, R, C), F32),
                pltpu.VMEM((R, 128), F32),
                pltpu.VMEM((R, 128), F32),
                pltpu.VMEM((R, 128), F32),
                pltpu.VMEM((R, 128), F32),
                pltpu.VMEM((NB, 3, 8, 128), F32),
                pltpu.VMEM((NB, 3, 8, 128), F32),
                pltpu.VMEM((NB, 8, 128), F32),
                pltpu.VMEM((NB, 8, 128), I32),
                DMA((8, 3)), DMA((8, 3)), DMA((8,)), DMA((8,)), DMA((2,)), DMA((8, 2)),
                DMA((NB,)), DMA((NB,)), DMA((NB, 3)), DMA((NB, 3)), DMA((NB,)), DMA((NB,)), DMA((2,)),
            ],
            compiler_params=params(0),
            cost_estimate=pl.CostEstimate(flops=2 * rows_all * D * C, bytes_accessed=120_000_000, transcendentals=rows_all * C),
            name="gather_logits",
        )(x, w, pieces(label))

        byx, g, part, _, _ = pl.pallas_call(
            second_kernel,
            out_shape=(
                S((R, D), BF16),
                S((rows_all, C), BF16),
                S((DONE * MB, C), BF16),
                S((8, R, D), BF16),
                S((8, R, D), BF16),
            ),
            in_specs=[ANY, ANY, ANY, VM, VM],
            out_specs=(ANY, ANY, ANY, ANY, ANY),
            scratch_shapes=[
                pltpu.VMEM((D, C), BF16),
                pltpu.VMEM((rows_all, C), BF16),
                pltpu.VMEM((2, 88, C), F32),
                pltpu.VMEM((7, R, D), BF16),
                pltpu.VMEM((R, 1536), F32),
                pltpu.VMEM((2, rows_all, MB), BF16),
                pltpu.VMEM((2, MB, C), BF16),
                pltpu.VMEM((R, 128), F32),
                pltpu.VMEM((R, 128), F32),
                pltpu.VMEM((R, 128), F32),
                DMA((1,)), DMA((2,)), DMA((2,)), DMA((8,)), DMA((5, 3)), DMA((8, 3)), DMA((8, 2)), DMA((8,)), DMA((2,)), DMA((2,)),
            ],
            compiler_params=params(1),
            cost_estimate=pl.CostEstimate(flops=3 * rows_all * D * C, bytes_accessed=200_000_000, transcendentals=rows_all * C),
            name="scatter_terms",
        )(z, xr, w, st, lab)

        by_w = pl.pallas_call(
            third_kernel,
            out_shape=S((D, C), BF16),
            in_specs=[ANY, ANY, ANY],
            out_specs=ANY,
            scratch_shapes=[
                pltpu.VMEM((rows_all, C), BF16),
                pltpu.VMEM((2, rows_all, MB), BF16),
                pltpu.VMEM((2, MB, C), BF16),
                pltpu.VMEM((DONE * MB, C), BF16),
                pltpu.VMEM((MB, C), F32),
                DMA((4,)), DMA((2,)), DMA((2,)), DMA((2,)),
            ],
            compiler_params=params(),
            cost_estimate=pl.CostEstimate(flops=rows_all * D * C, bytes_accessed=80_000_000, transcendentals=0),
            name="matrix_gradient",
        )(g, xr, part)

        loss = jnp.concatenate([loss[j, :n] for j, n in enumerate(PS)])
        return loss, byx, by_w

    return jax.shard_map(
        step,
        mesh=mesh,
        in_specs=(P(("dp", "tp"), None), P(None, "tp"), P(("dp", "tp"))),
        out_specs=(P(("dp", "tp")), P(("dp", "tp"), None), P("dp", "tp")),
        check_vma=False,
    )
```

```python
import jax
import jax.numpy as jnp
from jax import lax
from jax.experimental import pallas as pl
from jax.experimental.pallas import tpu as pltpu
from jax.sharding import PartitionSpec as P

F32, BF16, I32 = jnp.float32, jnp.bfloat16, jnp.int32
R, D, C = 352, 3072, 2048
H = R // 2
PO, PS = (0, 64, 128), (64, 64, 48)
AXES = (8, 4, 2)
NB = 16
MB = 256
DONE = 4
LAG = 10
VMEM_LIMIT = 67_000_000
THREE, TWO, PAIR = range(3), range(2), 2
LANES, Q = 128, 88
HALF_C, HALF_D = C // 2, D // 2


def flip(me, v):
    return v * (1 - 2 * ((me // v) % 2))


def place():
    me = lax.axis_index("tp")
    return me, me + flip(me, 1), [me + flip(me, v) for v in AXES]


def origin(me, s, k, j):
    q = me + k * flip(me, 1)
    for b in THREE:
        q = q + ((s // (1 << b)) % 2) * flip(me, AXES[(j + b) % 3])
    return q


def order(i):
    return jnp.where(i == 3, 4, jnp.where(i == 4, 3, i))


def rc(src, dst, ss, rs, dev):
    return pltpu.make_async_remote_copy(
        src_ref=src, dst_ref=dst, send_sem=ss, recv_sem=rs, device_id={"tp": dev}, device_id_type=pl.DeviceIdType.MESH
    )


def ds(start, size):
    return pl.ds(pl.multiple_of(start, 16), size)


def rows(j):
    return pl.ds(PO[j], PS[j])


def eye():
    return lax.broadcasted_iota(I32, (64, LANES), 0) == lax.broadcasted_iota(I32, (64, LANES), 1)


def to_column(row):
    return jnp.sum(jnp.where(eye(), row, 0.0), 1, keepdims=True)


def to_row(column, n):
    return jnp.sum(jnp.where(eye()[:n], column, 0.0), 0, keepdims=True)


def fill_columns(dst, k, tile, j, row, shift=0.0):
    put_column(dst, k, j, tile[pl.ds(row, 1), :].astype(F32) - shift)


def put_column(dst, k, j, row):
    col = to_column(row)
    dst[pl.ds(k * H + PO[j], PS[j]), :] = jnp.broadcast_to(col, (64, LANES))[: PS[j]]


def main_kernel(
    x_hbm, w_hbm, lab_ref,
    xr, z_hbm, loss_ref, g_hbm, bw, dbuf, ibuf, kept,
    w, g, acc, outd, outi, add, labc, c1, c2, c3, stile, strecv, st_all, lab_all,
    asend, arecv, adsend, adrecv, lsend, lrecv, ssend, srecv, tsend, trecv,
    dsend, drecv, isend, irecv, gsem, fsem, ksem, insem,
):
    me, partner, nbr = place()
    base = (me * C).astype(F32)
    barrier = pltpu.get_barrier_semaphore()

    def others(f):
        @pl.loop(1, NB)
        def _(t):
            f(t, (me + t) % NB)

    def own(h, b, j):
        n = h * 8 + (1 << b)
        return rc(
            x_hbm.at[ds(h * H + PO[j], PS[j])], xr.at[ds(n * R + PO[j], PS[j])],
            asend.at[n], arecv.at[n], nbr[(j + b) % 3],
        )

    def forward(h, s, b, j):
        n, t = h * 8 + s, h * 8 + s + (1 << b)
        return rc(
            xr.at[ds(n * R + PO[j], PS[j])], xr.at[ds(t * R + PO[j], PS[j])],
            asend.at[t], arecv.at[t], nbr[(j + b) % 3],
        )

    def pieces_of(n):
        return rc(xr.at[pl.ds(0, H)], xr.at[pl.ds(0, H)], asend.at[n], arecv.at[n], partner)

    def push(h, s):
        for b in (1, 2):

            @pl.when(s < (1 << b))
            def _():
                for j in THREE:
                    forward(h, s, b, j).start()

    def own_over(h):
        return rc(x_hbm.at[ds(h * H, H)], xr.at[ds(h * 8 * R + H, H)], adsend.at[h * 8], adrecv.at[h * 8], partner)

    def over(n):
        return rc(xr.at[ds(n * R, H)], xr.at[ds(n * R + H, H)], adsend.at[n], adrecv.at[n], partner)

    def label_copy(t, q):
        return rc(lab_ref, lab_all.at[me], lsend.at[0], lrecv.at[0], q)

    rest = pl.ds(0, NB - 1)

    def labels():
        return rc(lab_all.at[rest], lab_all.at[rest], lsend.at[0], lrecv.at[0], partner)

    def stat_copy(h, s, k, j):
        return rc(stile.at[h * 8 + s, k, j], strecv.at[h, me, j], ssend.at[h * 8 + s], srecv.at[h], origin(me, s, k, j))

    def top_copy(h, t, q):
        return rc(st_all.at[h, me], st_all.at[h, me], tsend.at[h], trecv.at[h], q)

    def tops(h):
        return rc(st_all.at[h, rest], st_all.at[h, rest], tsend.at[h], trecv.at[h], partner)

    def d2d(n, p):
        return rc(outd.at[p], dbuf.at[n], dsend.at[p], drecv.at[n], partner)

    def ici(n, b, p, j):
        return rc(outi.at[p, rows(j)], ibuf.at[n, rows(j)], isend.at[p], irecv.at[n], nbr[(j + b) % 3])

    def fetch(src, p):
        return pltpu.make_async_copy(src, add.at[p], fsem.at[p])

    def keep(h):
        return pltpu.make_async_copy(acc.at[1], kept.at[h], ksem.at[h])

    def g_out(n):
        return pltpu.make_async_copy(g.at[ds(n * R, R)], g_hbm.at[ds(n * R, R)], gsem.at[n])

    def wait_slot(n):
        rc(ibuf.at[n], ibuf.at[n], isend.at[0], irecv.at[n], partner).wait_recv()

    def wait_sent(p):
        rc(outi.at[p], ibuf.at[0], isend.at[p], irecv.at[0], partner).wait_send()

    def finish_start(v):
        s = 7 - order(v % 8)
        n = (v // 8) * 8 + s
        d2d(n, 0).wait_recv()
        fetch(dbuf.at[n], 0).start()

        @pl.when(s < 4)
        def _():
            wait_slot(n + 4)
            fetch(ibuf.at[n + 4], 1).start()

        @pl.when(s < 2)
        def _():
            wait_slot(n + 2)
            fetch(ibuf.at[n + 2], 2).start()

    def finish(v):
        s = 7 - order(v % 8)
        n = (v // 8) * 8 + s
        p = v % 3

        @pl.when(v > 2)
        def _():
            wait_sent(p)

        fetch(dbuf.at[n], 0).wait()

        def total(count):
            @pl.loop(0, H // 16)
            def _(i):
                r = pl.ds(pl.multiple_of(i * 16, 16), 16)
                out = acc[v % 2, r, :]
                for q in range(count):
                    out = out + add[q, r, :].astype(F32)
                outi[p, r, :] = out.astype(BF16)

        @pl.when(s >= 4)
        def _():
            total(1)
            for j in THREE:
                ici(n, 2, p, j).start()

        @pl.when(s < 4)
        def _():
            fetch(dbuf.at[n], 1).wait()

        @pl.when((s >= 2) & (s < 4))
        def _():
            total(2)
            for j in THREE:
                ici(n, 1, p, j).start()

        @pl.when(s == 1)
        def _():
            fetch(dbuf.at[n], 2).wait()
            total(3)
            for j in THREE:
                ici(n, 0, p, j).start()

    def combine(h):
        rc(strecv.at[h, rest], strecv.at[h, rest], ssend.at[0], srecv.at[h], partner).wait_recv()
        for j in THREE:
            tiles = [strecv[h, q, j] for q in range(NB)]
            top = tiles[0][0:1]
            for t in tiles[1:]:
                top = jnp.maximum(top, t[0:1])
            total = jnp.zeros((1, LANES), F32)
            right = jnp.zeros((1, LANES), F32)
            for t in tiles:
                total = total + t[1:2] * jnp.exp(t[0:1] - top)
                right = right + t[2:3]
            loss_ref[h, j : j + 1, :] = jnp.log(total) + top - right
            st_all[h, me, j : j + 1, :] = top
            st_all[h, me, j + 3 : j + 4, :] = 1.0 / total
        others(lambda t, q: top_copy(h, t, q).start())

    def passes(xbuf, zb, zin, xsem, zosem, zisem):
        def load_w(c):
            cols = pl.ds(pl.multiple_of(c * HALF_C, HALF_C), HALF_C)
            return pltpu.make_async_copy(w_hbm.at[:, cols], w.at[:, cols], insem.at[c])

        load_own = pltpu.make_async_copy(x_hbm, xbuf.at[1], insem.at[4])

        def put_own(h):
            return pltpu.make_async_copy(xbuf.at[1, pl.ds(h * H, H)], xr.at[ds(h * 8 * R, H)], insem.at[2 + h])

        def x_load(n, par):
            return pltpu.make_async_copy(xr.at[ds(n * R, R)], xbuf.at[par], xsem.at[par])

        def x_half(n, k, par):
            return pltpu.make_async_copy(xr.at[ds(n * R + k * H, H)], xbuf.at[par, pl.ds(k * H, H)], xsem.at[par])

        def z_out(n, par):
            return pltpu.make_async_copy(zb.at[par], z_hbm.at[ds(n * R, R)], zosem.at[par])

        def z_in(n, q):
            return pltpu.make_async_copy(z_hbm.at[pl.ds(pl.multiple_of(n * R + q * Q, 8), Q)], zin.at[q], zisem.at[q])

        load_own.start()
        first = pltpu.make_async_copy(x_hbm.at[pl.ds(0, H)], xbuf.at[0, pl.ds(0, H)], xsem.at[0])
        first.start()
        for c in TWO:
            load_w(c).start()
        others(lambda t, q: pl.semaphore_signal(barrier, inc=1, device_id={"tp": q}, device_id_type=pl.DeviceIdType.MESH))
        pl.semaphore_wait(barrier, NB - 1)
        own_over(0).start()
        others(lambda t, q: label_copy(t, q).start())
        for b in THREE:
            for j in THREE:
                own(0, b, j).start()
        lab_all[me] = lab_ref[...]
        load_own.wait()
        for h in TWO:
            put_own(h).start()
        own_over(0).wait_recv()
        pltpu.make_async_copy(xr.at[pl.ds(H, H)], xbuf.at[0, pl.ds(H, H)], xsem.at[0]).start()
        for h in TWO:
            put_own(h).wait()

        @pl.loop(0, 16 + LAG)
        def _(t):
            @pl.when(t < 16)
            def _():
                h = t // 8
                s = order(t % 8)
                n = h * 8 + s
                par = t % 2
                t1 = jnp.minimum(t + 1, 15)
                n1 = (t1 // 8) * 8 + order(t1 % 8)
                t2 = jnp.where(t < 7, t + 1, t + 2)
                h2 = jnp.minimum(t2 // 8, 1)
                s2 = order(t2 % 8)
                n2 = h2 * 8 + s2
                x_load(n, par).wait()

                @pl.when((t >= 7) & (t < 15))
                def _():
                    over(n1).wait_recv()
                    x_half(n1, 0, 1 - par).start()
                    x_half(n1, 1, 1 - par).start()

                @pl.when(t > 1)
                def _():
                    z_out(0, par).wait()

                @pl.when(t == 0)
                def _():
                    load_w(0).wait()
                    load_w(1).wait()

                @pl.loop(0, PAIR)
                def _(c):
                    cols = pl.ds(pl.multiple_of(c * HALF_C, HALF_C), HALF_C)
                    zb[par, :, cols] = jnp.dot(xbuf[par], w[:, cols], preferred_element_type=F32)

                @pl.when((t2 < 16) & (s2 > 0))
                def _():
                    pieces_of(n2).wait_recv()

                    @pl.when(t < 7)
                    def _():
                        push(h2, s2)
                        x_half(n1, 0, 1 - par).start()

                    over(n2).start()

                @pl.when(t == 5)
                def _():
                    own_over(1).start()
                    for j in THREE:
                        own(1, 0, j).start()

                @pl.when(t == 0)
                def _():
                    labels().wait_recv()

                for k in TWO:
                    for j in THREE:
                        fill_columns(labc, k, lab_all.at[origin(me, s, k, j)], j, h * 3 + j, base)

                @pl.loop(0, 4)
                def _(i):
                    r = pl.ds(pl.multiple_of(i * Q, 8), Q)
                    high = zb[par, r, 0:LANES]
                    for c in range(1, C // LANES):
                        high = jnp.maximum(high, zb[par, r, c * LANES : (c + 1) * LANES])
                    high = jnp.max(high, 1, keepdims=True)
                    lab = labc[r, :]
                    lane = lax.broadcasted_iota(I32, (1, LANES), 1).astype(F32)
                    sums = jnp.zeros((Q, LANES), F32)
                    right = jnp.zeros((Q, LANES), F32)
                    for c in range(C // LANES):
                        z = zb[par, r, c * LANES : (c + 1) * LANES]
                        e = jnp.exp(z - high)
                        hit = lane + float(c * LANES) == lab
                        sums = sums + e
                        right = right + jnp.where(hit, z, 0.0)
                        zb[par, r, c * LANES : (c + 1) * LANES] = jnp.where(hit, -1e-30 - e, e)
                    c1[r, :] = jnp.broadcast_to(high, (Q, LANES))
                    c2[r, :] = jnp.broadcast_to(jnp.sum(sums, 1, keepdims=True), (Q, LANES))
                    c3[r, :] = jnp.broadcast_to(jnp.sum(right, 1, keepdims=True), (Q, LANES))

                z_out(n, par).start()
                for k in TWO:
                    for j in THREE:
                        for i, ref in enumerate((c1, c2, c3)):
                            stile[n, k, j, i : i + 1, :] = to_row(ref[pl.ds(k * H + PO[j], PS[j]), :], PS[j])

                @pl.when(s == 0)
                def _():
                    for j in THREE:
                        strecv[h, me, j] = stile[n, 0, j]

                @pl.when(s > 0)
                def _():
                    for j in THREE:
                        stat_copy(h, s, 0, j).start()

                for j in THREE:
                    stat_copy(h, s, 1, j).start()

                @pl.when(t < 7)
                def _():
                    over(n1).wait_recv()
                    x_half(n1, 1, 1 - par).start()

            for b in (1, 2):

                @pl.when(t == 5 + b)
                def _():
                    for j in THREE:
                        own(1, b, j).start()

            @pl.when(t == 8)
            def _():
                combine(0)
                push(1, 1)

            @pl.when((t >= 8) & (t < 14))
            def _():
                push(1, order((t + 2) % 8))

            @pl.when(t == LAG - 1)
            def _():
                for i in range(4):
                    z_in(7, i).start()

            @pl.when(t == 16)
            def _():
                combine(1)
                z_out(0, 0).wait()
                z_out(0, 1).wait()

            @pl.when(t >= LAG)
            def _():
                u = t - LAG
                h = u // 8
                s = 7 - order(u % 8)
                n = h * 8 + s
                a = u % 2
                u2 = jnp.minimum(u + 1, 15)
                n2 = (u2 // 8) * 8 + 7 - order(u2 % 8)
                v = jnp.maximum(u - 1, 0)
                send_on = (u > 0) & (u != 8) & (u != 15)

                @pl.when(u % 8 == 0)
                def _():
                    tops(h).wait_recv()

                for k in TWO:
                    for j in THREE:
                        q = origin(me, s, k, j)
                        scale = jnp.exp(stile[n, k, j, 0:1, :] - st_all[h, q, j : j + 1, :]) * st_all[h, q, j + 3 : j + 4, :]
                        put_column(c1, k, j, scale)

                @pl.loop(0, 4)
                def _(i):
                    z_in(n, i).wait()
                    r = pl.ds(pl.multiple_of(i * Q, 8), Q)
                    to = pl.ds(pl.multiple_of(n * R + i * Q, 8), Q)
                    scale = c1[r, :]
                    for c in range(C // LANES):
                        e = zin[i, :, c * LANES : (c + 1) * LANES]
                        p = e * scale
                        g[to, c * LANES : (c + 1) * LANES] = jnp.where(e < 0.0, -1.0 - p, p).astype(BF16)

                    @pl.when(u < 15)
                    def _():
                        z_in(n2, i).start()

                g_out(n).start()

                @pl.when(u > 1)
                def _():
                    d2d(0, a).wait_send()

                @pl.when(u == 9)
                def _():
                    keep(0).wait()

                @pl.loop(0, PAIR)
                def _(c):
                    @pl.when((c == 1) & send_on)
                    def _():
                        finish_start(v)

                    cols = pl.ds(pl.multiple_of(c * HALF_D, HALF_D), HALF_D)
                    term = lax.dot_general(
                        g[ds(n * R, R), :], w[cols, :], (((1,), (1,)), ((), ())), preferred_element_type=F32
                    )
                    acc[a, :, cols] = term[:H]
                    outd[a, :, cols] = term[H:].astype(BF16)

                d2d(n, a).start()

                @pl.when(u % 8 == 7)
                def _():
                    keep(h).start()

                @pl.when(send_on)
                def _():
                    finish(v)

    def under(xb, ob, xsem, osem):
        def x_in(m):
            return pltpu.make_async_copy(xr.at[:, pl.ds(m * MB, MB)], xb.at[m % 2], xsem.at[m % 2])

        def bw_out(m):
            return pltpu.make_async_copy(ob.at[m % 2], bw.at[pl.ds(m * MB, MB)], osem.at[m % 2])

        x_in(0).start()
        x_in(1).start()

        finish_start(jnp.int32(14))

        @pl.loop(0, DONE)
        def _(m):
            x_in(m).wait()

            @pl.when(m > 1)
            def _():
                bw_out(m - 2).wait()

            by_w_block(xb.at[m % 2], g, ob.at[m % 2])
            bw_out(m).start()

            @pl.when(m + 2 < DONE)
            def _():
                x_in(m + 2).start()

            @pl.when(m == 0)
            def _():
                finish(jnp.int32(14))

        for m in (DONE - 2, DONE - 1):
            bw_out(m).wait()

    sem = pltpu.SemaphoreType.DMA
    pl.run_scoped(passes, pltpu.VMEM((2, R, D), BF16), pltpu.VMEM((2, R, C), F32), pltpu.VMEM((4, Q, C), F32), sem((2,)), sem((2,)), sem((4,)))
    pl.run_scoped(under, pltpu.VMEM((2, NB * R, MB), BF16), pltpu.VMEM((2, MB, C), BF16), sem((2,)), sem((2,)))

    for a in TWO:
        d2d(0, a).wait_send()
    keep(1).wait()
    for h in TWO:
        d2d(h * 8, 0).wait_recv()
        for s in (1, 2, 4):
            wait_slot(h * 8 + s)

    for p in THREE:
        wait_sent(p)

    @pl.loop(0, 16)
    def _(n):
        g_out(n).wait()
        over(n).wait_send()

        @pl.when(n % 8 > 0)
        def _():
            pieces_of(n).wait_send()
            rc(stile.at[n], stile.at[n], ssend.at[n], srecv.at[0], partner).wait_send()

        @pl.when(n % 8 == 0)
        def _():
            rc(stile.at[n, 1], stile.at[n, 1], ssend.at[n], srecv.at[0], partner).wait_send()

    labels().wait_send()
    for h in TWO:
        tops(h).wait_send()


def by_w_block(xb, g, ob):
    for c in range(4):
        ob[:, c * 512 : (c + 1) * 512] = lax.dot_general(
            xb[...], g[:, c * 512 : (c + 1) * 512], (((0,), (0,)), ((), ())), preferred_element_type=F32
        ).astype(BF16)


def third_kernel(
    g_hbm, xr_hbm, part_hbm, kept, dbuf, ibuf,
    bw, byx,
    g, xb, ob, part, acc, sums, add, gsem, x0sem, xsem, osem, psem, fsem, ysem,
):
    blocks = D // MB
    cuts = ((0, 512), (512, 1024), (1536, 2048), (3584, 2048))

    def g_in(n):
        r = pl.ds(*cuts[n])
        return pltpu.make_async_copy(g_hbm.at[r], g.at[r], gsem.at[n])

    def x_cut(i, n):
        r = pl.ds(*cuts[n])
        return pltpu.make_async_copy(xr_hbm.at[r, pl.ds((DONE + i) * MB, MB)], xb.at[i, r], x0sem.at[i, n])

    def x_in(m):
        return pltpu.make_async_copy(xr_hbm.at[:, pl.ds(m * MB, MB)], xb.at[m % 2], xsem.at[m % 2])

    def bw_out(m):
        return pltpu.make_async_copy(ob.at[m % 2], bw.at[pl.ds(m * MB, MB)], osem.at[m % 2])

    p_in = pltpu.make_async_copy(part_hbm, part, psem.at[0])
    p_out = pltpu.make_async_copy(part, bw.at[pl.ds(0, DONE * MB)], psem.at[1])
    came = [pltpu.make_async_copy(kept, sums, fsem.at[8])]
    for h in TWO:
        came.append(pltpu.make_async_copy(dbuf.at[h * 8], add.at[h, 0], fsem.at[h * 4]))
        for p, n in enumerate((1, 2, 4)):
            came.append(pltpu.make_async_copy(ibuf.at[h * 8 + n], add.at[h, p + 1], fsem.at[h * 4 + p + 1]))
    y_out = [pltpu.make_async_copy(add.at[h, 0], byx.at[pl.ds(h * H, H)], ysem.at[h]) for h in TWO]

    def begin(n):
        for i in TWO:
            x_cut(i, n).start()
        g_in(n).start()

    begin(0)
    begin(1)
    for n in range(4):
        r = pl.ds(*cuts[n])
        for i in TWO:
            x_cut(i, n).wait()
        g_in(n).wait()
        if n < 2:
            begin(n + 2)
        for i in TWO:

            @pl.loop(0, PAIR)
            def _(c):
                cols = pl.ds(pl.multiple_of(c * HALF_C, HALF_C), HALF_C)
                t = lax.dot_general(xb[i, r, :], g[r, cols], (((0,), (0,)), ((), ())), preferred_element_type=F32)
                if n == 0:
                    acc[i, :, cols] = t
                elif n < 3:
                    acc[i, :, cols] += t
                else:
                    ob[i, :, cols] = (acc[i, :, cols] + t).astype(BF16)

            if n == 3:
                bw_out(DONE + i).start()
                x_in(DONE + 2 + i).start()
    p_in.start()
    for copy in came:
        copy.start()

    @pl.loop(DONE + 2, blocks)
    def _(m):
        x_in(m).wait()
        bw_out(m - 2).wait()
        by_w_block(xb.at[m % 2], g, ob.at[m % 2])
        bw_out(m).start()

        @pl.when(m + 2 < blocks)
        def _():
            x_in(m + 2).start()

        @pl.when(m == DONE + 4)
        def _():
            p_in.wait()
            p_out.start()
            for copy in came:
                copy.wait()
            for h in TWO:

                @pl.loop(0, H // 16)
                def _(i):
                    r = pl.ds(pl.multiple_of(i * 16, 16), 16)
                    out = sums[h, r, :]
                    for p in range(4):
                        out = out + add[h, p, r, :].astype(F32)
                    add[h, 0, r, :] = out.astype(BF16)

                y_out[h].start()

    for m in (blocks - 2, blocks - 1):
        bw_out(m).wait()
    p_out.wait()
    for copy in y_out:
        copy.wait()


ANY = pl.BlockSpec(memory_space=pl.ANY)
VM = pl.BlockSpec(memory_space=pltpu.VMEM)


def params(n=None):
    if n is None:
        return pltpu.CompilerParams(vmem_limit_bytes=VMEM_LIMIT)
    return pltpu.CompilerParams(vmem_limit_bytes=VMEM_LIMIT, collective_id=n, has_side_effects=True)


def S(shape, dtype):
    return jax.ShapeDtypeStruct(shape, dtype)


def pieces(v):
    v = jnp.pad(v.reshape(2, H), ((0, 0), (0, 16))).reshape(6, 64)
    return jnp.pad(v, ((0, 2), (0, 64)))


def solution(mesh):
    DMA = pltpu.SemaphoreType.DMA
    rows_all = NB * R

    def step(x, w, label):
        xr, _, loss, g, part, dbuf, ibuf, kept = pl.pallas_call(
            main_kernel,
            out_shape=(
                S((rows_all, D), BF16),
                S((rows_all, C), F32),
                S((2, 8, LANES), F32),
                S((rows_all, C), BF16),
                S((DONE * MB, C), BF16),
                S((16, H, D), BF16),
                S((16, H, D), BF16),
                S((2, H, D), F32),
            ),
            in_specs=[ANY, ANY, VM],
            out_specs=(ANY, ANY, VM, ANY, ANY, ANY, ANY, ANY),
            scratch_shapes=[
                pltpu.VMEM((D, C), BF16),
                pltpu.VMEM((rows_all, C), BF16),
                pltpu.VMEM((2, H, D), F32),
                pltpu.VMEM((2, H, D), BF16),
                pltpu.VMEM((3, H, D), BF16),
                pltpu.VMEM((3, H, D), BF16),
                pltpu.VMEM((R, LANES), F32),
                pltpu.VMEM((R, LANES), F32),
                pltpu.VMEM((R, LANES), F32),
                pltpu.VMEM((R, LANES), F32),
                pltpu.VMEM((16, 2, 3, 8, LANES), F32),
                pltpu.VMEM((2, NB, 3, 8, LANES), F32),
                pltpu.VMEM((2, NB, 8, LANES), F32),
                pltpu.VMEM((NB, 8, LANES), I32),
                *[DMA((n,)) for n in (16, 16, 16, 16, 1, 1, 16, 2, 2, 2, 2, 16, 3, 16)], DMA((16,)), DMA((3,)), DMA((2,)), DMA((5,)),
            ],
            compiler_params=params(0),
            cost_estimate=pl.CostEstimate(flops=5 * rows_all * D * C, bytes_accessed=300_000_000, transcendentals=2 * rows_all * C),
            name="gather_logits_terms",
        )(x, w, pieces(label))

        by_w, byx = pl.pallas_call(
            third_kernel,
            out_shape=(S((D, C), BF16), S((R, D), BF16)),
            in_specs=[ANY] * 6,
            out_specs=(ANY, ANY),
            scratch_shapes=[
                pltpu.VMEM((rows_all, C), BF16),
                pltpu.VMEM((2, rows_all, MB), BF16),
                pltpu.VMEM((2, MB, C), BF16),
                pltpu.VMEM((DONE * MB, C), BF16),
                pltpu.VMEM((2, MB, C), F32),
                pltpu.VMEM((2, H, D), F32),
                pltpu.VMEM((2, 4, H, D), BF16),
                DMA((4,)), DMA((2, 4)), DMA((2,)), DMA((2,)), DMA((2,)), DMA((9,)), DMA((2,)),
            ],
            compiler_params=params(),
            cost_estimate=pl.CostEstimate(flops=rows_all * D * C, bytes_accessed=80_000_000, transcendentals=0),
            name="matrix_gradient",
        )(g, xr, part, kept, dbuf, ibuf)

        loss = loss[:, :3, :64].reshape(2, 192)[:, :H].reshape(R)
        return loss, byx, by_w

    return jax.shard_map(
        step,
        mesh=mesh,
        in_specs=(P(("dp", "tp"), None), P(None, "tp"), P(("dp", "tp"))),
        out_specs=(P(("dp", "tp")), P(("dp", "tp"), None), P("dp", "tp")),
        check_vma=False,
    )
```
